128 devices in a mesh: trade: 4 (over z), node: 32 (over x, y, core).
Axes of the slice: x: 4, y: 4, z: 4, core: 2. Of those that a mesh axis runs over, the one named last changes fastest.
Arguments:
- values_in: float32 [1024, 65536], P('trade', 'node'), may hold values from 0 to 1
- prob_up: float32 [16, 65536], P(None, 'node'), may hold values from 0.1 to 0.3
- prob_down: float32 [16, 65536], P(None, 'node'), may hold values from 0.1 to 0.3
- discount: float32 [16, 65536], P(None, 'node'), may hold values from 0.9 to 1
- swap_rate: float32 [16, 65536], P(None, 'node'), may hold values from -3 to 3
- annuity: float32 [16, 65536], P(None, 'node'), may hold values from 0.5 to 2
- state_price: float32 [65536], P('node'), may hold values from 7.6293945e-06 to 3.0517578e-05
- exercise_step: int32 [1024, 4], P('trade'), may hold values from 0 to 15
- strike_bucket: int32 [1024], P('trade'), may hold values from 0 to 63
- notional_sign: int32 [1024], P('trade'), may hold values from 0 to 1
- strike_table: float32 [64], replicated, may hold values from -0.5 to 0.5
Outputs:
- values_out: float32 [1024, 65536], P(('trade', 'node'))
- prices: float32 [1024], P(('trade', 'node'))
- portfolio: float32 [], replicated
The draws below stay inside these ranges and needn't reach their ends.
All inputs are finite; a program needn't handle non-finite values.
Results may differ from the reference program's by a relative error of at most 0.0003.
Values sent between devices are 32-bit elements; how exact they have to be, the bound alone decides.
No kernel may reach another device: no remote copies, remote signals or barrier semaphores. Data moves between devices by JAX's collectives and lax.ppermute only.
A program may use at most 128 MiB of HBM per device.

```python
import math
import jax
import jax.numpy as jnp
from jax import lax

TRADE_DEV = 256
STEPS = 16
EXDATES = 4
BUCKETS = 64
NODES = 65536
TRADES = 1024
N_TRADE = 4


def touch_ends(drawn, stream_key, low, top_value):
    shape = drawn.shape
    index_at = [jax.random.randint(jax.random.fold_in(stream_key, axis), (), 0, shape[axis]) for axis in range(len(shape))]
    drawn = drawn.at[tuple(index_at)].set(low)
    longest = shape.index(max(shape))
    index_at[longest] = (index_at[longest] + 1) % shape[longest]
    return drawn.at[tuple(index_at)].set(top_value)


def block_levels(rng, shape, cuts, least, largest):
    level, own = 1.0, jax.random.fold_in(rng, 6)
    for axis_at, shards_of in cuts:
        heights = jnp.exp(jax.random.uniform(jax.random.fold_in(own, axis_at), (shards_of,), jnp.float32, least / len(cuts), largest / len(cuts)))
        level = level * jnp.repeat(heights, shape[axis_at] // shards_of).reshape([-1 if axis == axis_at else 1 for axis in range(len(shape))])
    return level


def normal_values(own_key, dims, deviation, most, cuts=(), held_as=jnp.bfloat16):
    entries = jax.random.normal(own_key, dims, jnp.float32) * deviation
    if len(cuts) > 0:
        entries = block_levels(own_key, dims, cuts, -0.22, 0.18) * entries
    return jnp.clip(entries, min=-most, max=most).astype(held_as)


def setup_inputs(seed: int = 0) -> dict:
    arg_keys = jax.random.split(jax.random.key(seed), 12)
    values_in = jnp.clip(1.0 * jax.random.uniform(arg_keys[0], (TRADES, NODES), jnp.float32) ** block_levels(arg_keys[0], (TRADES, NODES), ((0, 4), (1, 32)), -0.2, 0.2), 0.0, 1.0)
    prob_up = jnp.clip(0.1 + 0.20000001043081284 * jax.random.uniform(arg_keys[1], (STEPS, NODES), jnp.float32) ** block_levels(arg_keys[1], (STEPS, NODES), ((1, 32),), -0.2, 0.2), 0.1, 0.3)
    prob_down = jnp.clip(0.1 + 0.20000001043081284 * jax.random.uniform(arg_keys[2], (STEPS, NODES), jnp.float32) ** block_levels(arg_keys[2], (STEPS, NODES), ((1, 32),), -0.2, 0.2), 0.1, 0.3)
    discount = jnp.clip(0.9 + 0.100000024 * jax.random.uniform(arg_keys[3], (STEPS, NODES), jnp.float32) ** block_levels(arg_keys[3], (STEPS, NODES), ((1, 32),), -0.2, 0.2), 0.9, 1.0)
    swap_rate = normal_values(arg_keys[4], (STEPS, NODES), 0.5, 3.0, ((1, 32),), jnp.float32)
    annuity = jnp.clip(jnp.exp(math.log(2.0) - 1.3862944 * jax.random.uniform(arg_keys[5], (STEPS, NODES), jnp.float32) ** block_levels(arg_keys[5], (STEPS, NODES), ((1, 32),), -0.2, 0.2)), 0.5, 2.0)
    state_price = jnp.clip(jnp.exp(math.log(3.0517578125e-05) - 1.3862944 * jax.random.uniform(arg_keys[6], (NODES,), jnp.float32) ** block_levels(arg_keys[6], (NODES,), ((0, 32),), -0.2, 0.2)), 7.62939453125e-06, 3.0517578125e-05)
    exercise_step = touch_ends(jax.random.randint(arg_keys[7], (TRADES, EXDATES), 0, STEPS), jax.random.fold_in(arg_keys[7], 1), 0, STEPS - 1).astype(jnp.int32)
    strike_bucket = touch_ends(jax.random.randint(arg_keys[8], (TRADES,), 0, BUCKETS), jax.random.fold_in(arg_keys[8], 1), 0, BUCKETS - 1).astype(jnp.int32)
    notional_sign = touch_ends(jax.random.randint(arg_keys[9], (TRADES,), 0, 2), jax.random.fold_in(arg_keys[9], 1), 0, 1).astype(jnp.int32)
    strike_table = jnp.clip(jax.random.uniform(arg_keys[10], (BUCKETS,), jnp.float32, -0.5, 0.5), -0.5, 0.5)
    return {"values_in": values_in, "prob_up": prob_up, "prob_down": prob_down, "discount": discount, "swap_rate": swap_rate, "annuity": annuity, "state_price": state_price, "exercise_step": exercise_step, "strike_bucket": strike_bucket, "notional_sign": notional_sign, "strike_table": strike_table}


def strikes_of(bucket, strike_table):
    levels = lax.broadcasted_iota(jnp.int32, (1, strike_table.shape[0]), 1)
    return jnp.sum(jnp.where(bucket[:, None] == levels, strike_table[None, :], jnp.zeros((), strike_table.dtype)), axis=1)


def roll_once(padded, prob_up, prob_down, discount_row):
    middle = 1.0 - prob_up - prob_down
    return discount_row * (prob_up * padded[:, 2:] + middle * padded[:, 1:-1] + prob_down * padded[:, :-2])


def exercise(values, active, strike, signs, swap_row, annuity_row):
    payoff = signs[:, None] * annuity_row[None, :] * (swap_row[None, :] - strike[:, None])
    return jnp.where(active[:, None], jnp.maximum(values, payoff), values)


def reference(values_in, prob_up, prob_down, discount, swap_rate, annuity, state_price, exercise_step, strike_bucket, notional_sign, strike_table):
    strike = strikes_of(strike_bucket, strike_table)
    signs = (2 * notional_sign - 1).astype(jnp.float32)

    def one_block(pieces):
        values, dates, strikes, sign_rows = pieces
        for step in range(STEPS):
            padded = jnp.pad(values, ((0, 0), (1, 1)))
            values = roll_once(padded, prob_up[step], prob_down[step], discount[step])
            active = jnp.any(dates == step, axis=1)
            values = exercise(values, active, strikes, sign_rows, swap_rate[step], annuity[step])
        block_prices = jnp.sum(values * state_price[None, :], axis=1)
        return values, block_prices

    shaped = (values_in.reshape(N_TRADE, TRADE_DEV, NODES), exercise_step.reshape(N_TRADE, TRADE_DEV, EXDATES), strike.reshape(N_TRADE, TRADE_DEV), signs.reshape(N_TRADE, TRADE_DEV))
    values_all, prices_all = lax.map(one_block, shaped)
    prices = prices_all.reshape(TRADES)
    portfolio = jnp.sum(prices) / TRADE_DEV
    return values_all.reshape(TRADES, NODES), prices, portfolio
```

```python
import functools

import jax
import jax.numpy as jnp
from jax import lax
from jax.experimental import pallas as pl
from jax.experimental.pallas import tpu as pltpu
from jax.sharding import Mesh
from jax.sharding import PartitionSpec as P

LANES = 128
ROWS = 8
OFF = 1e30
TRADE = ("trade_0", "trade_1")
NODE = ("x_0", "x_1", "y_0", "y_1", "core")
TRADE_NODE = TRADE + NODE


def scaled_rows(up, down, disc, ann):
    row = lax.broadcasted_iota(jnp.int32, ann.shape, 0)
    width = ann.shape[1]
    before = jnp.where(row == 0, 1.0, pltpu.roll(ann, 1, 0))
    share = disc / ann
    a = share * up * pltpu.roll(before, width - 1, 1)
    b = share * (1.0 - up - down) * before
    c = share * down * pltpu.roll(before, 1, 1)
    return a, b, c


def trade_columns(ex_ref, bucket_ref, sign_ref, table_ref, half):
    ex = ex_ref[:, half * LANES : (half + 1) * LANES]
    bits = jnp.left_shift(jnp.ones_like(ex), ex)
    mask = bits[0:1] | bits[1:2] | bits[2:3] | bits[3:4]
    bucket = bucket_ref[half : half + 1, :]
    levels = lax.broadcasted_iota(jnp.int32, (table_ref.shape[1], LANES), 0)
    strike = jnp.dot(
        table_ref[...],
        (levels == bucket).astype(jnp.float32),
        precision=lax.Precision.HIGHEST,
        preferred_element_type=jnp.float32,
    )
    sign = (2 * sign_ref[half : half + 1, :] - 1).astype(jnp.float32)

    def column(r):
        return jnp.transpose(jnp.broadcast_to(r, (LANES, LANES)))

    return column(sign), column(sign * strike), column(mask.astype(jnp.float32)).astype(jnp.int32)


def on_terms(sign, key, mask, step):
    on = (mask & (1 << step)) != 0
    return jnp.where(on, sign, 0.0), jnp.where(on, key, OFF)


def pack_kernel(v_ref, up_ref, dn_ref, dc_ref, sr_ref, an_ref, sp_ref, out_ref):
    n, steps = v_ref.shape[0], up_ref.shape[0]
    out_ref[0:n, :] = v_ref[...]
    for i, ref in enumerate((up_ref, dn_ref, dc_ref, sr_ref, an_ref)):
        out_ref[n + i * steps : n + (i + 1) * steps, :] = ref[...]
    out_ref[n + 5 * steps : n + 5 * steps + ROWS, :] = jnp.broadcast_to(sp_ref[0:1, :], (ROWS, LANES))


def interior_kernel(
    groups, v_ref, up_ref, dn_ref, dc_ref, sr_ref, an_ref, sp_ref, ex_ref, bk_ref, sg_ref, tb_ref,
    out_ref, acc_ref, sgn_out, key_out, mask_out,
    nat_ref, coef_ref, x_ref, node_ref, buf_ref,
):
    steps, width = up_ref.shape
    tiles = width // LANES
    block = v_ref.shape[0]
    rows = groups * ROWS
    i = pl.program_id(0)

    def spread(src, dst, count):
        for t in range(tiles):
            node_ref[t * LANES : (t + 1) * LANES, 0:count] = jnp.transpose(
                src[0:count, t * LANES : (t + 1) * LANES]
            )
        for k in range(tiles):
            dst[0:count, k * LANES : (k + 1) * LANES] = jnp.transpose(
                node_ref[pl.ds(k, LANES, stride=tiles), 0:count]
            )

    @pl.when(i == 0)
    def _():
        a, b, c = scaled_rows(up_ref[...], dn_ref[...], dc_ref[...], an_ref[...])
        for j, z in enumerate((a, b, c, sr_ref[...])):
            nat_ref[j * steps : (j + 1) * steps, :] = z
        nat_ref[4 * steps : 4 * steps + ROWS, :] = an_ref[steps - ROWS : steps, :]
        for t in range(tiles):
            nat_ref[4 * steps + ROWS : 4 * steps + 2 * ROWS, t * LANES : (t + 1) * LANES] = jnp.broadcast_to(
                sp_ref[t : t + 1, :], (ROWS, LANES)
            )
        nat_ref[4 * steps + 2 * ROWS :, :] = jnp.zeros((LANES - 4 * steps - 2 * ROWS, width), jnp.float32)
        spread(nat_ref, coef_ref, LANES)
        for half in range(2):
            sign, key, mask = trade_columns(ex_ref, bk_ref, sg_ref, tb_ref, half)
            at = pl.ds(half * LANES, LANES)
            sgn_out[at, :] = sign
            key_out[at, :] = key
            mask_out[at, :] = mask

    spread(v_ref, x_ref, block)
    lane = lax.broadcasted_iota(jnp.int32, (ROWS, LANES), 1)
    own = (lane > 0) & (lane < LANES - 1)

    @pl.loop(0, block // rows)
    def _(g):
        at = [pl.ds(pl.multiple_of(g * rows + ROWS * q, ROWS), ROWS) for q in range(groups)]
        base = [pl.ds(pl.multiple_of(i * block + g * rows + ROWS * q, ROWS), ROWS) for q in range(groups)]
        sign = [sgn_out[z, :] for z in base]
        key = [key_out[z, :] for z in base]
        mask = [mask_out[z, :] for z in base]

        def wide(r, k):
            return jnp.broadcast_to(coef_ref[r : r + 1, k * LANES : (k + 1) * LANES], (ROWS, LANES))

        def load(s, q, k):
            cols = slice(k * LANES, (k + 1) * LANES)
            return x_ref[at[q], cols] if s == 0 else buf_ref[(s - 1) % 2, ROWS * q : ROWS * (q + 1), cols]

        acc = [jnp.zeros((ROWS, LANES), jnp.float32)] * groups
        ends = [[load(0, q, 0), load(0, q, tiles - 1)] for q in range(groups)]
        for s in range(steps):
            terms = [on_terms(sign[q], key[q], mask[q], s) for q in range(groups)]
            up = [pltpu.roll(ends[q][0], LANES - 1, 1) for q in range(groups)]
            dn = [pltpu.roll(ends[q][1], 1, 1) for q in range(groups)]
            mid, nxt = [None] * groups, [None] * groups
            for k in [tiles - 1] + list(range(tiles - 1)):
                a, b, c, p = (wide(j * steps + s, k) for j in range(4))
                if s == steps - 1:
                    fin, price = wide(4 * steps + ROWS - 1, k), wide(4 * steps + ROWS, k)
                for q in range(groups):
                    if k == tiles - 1:
                        below, here, above = load(s, q, k - 1), load(s, q, k), up[q]
                    elif k == 0:
                        below, here, above = dn[q], load(s, q, 0), load(s, q, 1)
                        mid[q], nxt[q] = here, above
                    else:
                        below, here, above = mid[q], nxt[q], load(s, q, k + 1)
                        mid[q], nxt[q] = here, above
                    alpha, beta = terms[q]
                    new = jnp.maximum(a * above + b * here + c * below, alpha * p - beta)
                    cols = slice(k * LANES, (k + 1) * LANES)
                    if s == steps - 1:
                        new = new * fin
                        x_ref[at[q], cols] = new
                        acc[q] = acc[q] + new * price
                    else:
                        buf_ref[s % 2, ROWS * q : ROWS * (q + 1), cols] = new
                    if k == 0:
                        ends[q][0] = new
                    if k == tiles - 1:
                        ends[q][1] = new
        for q in range(groups):
            acc_ref[at[q], :] = jnp.where(own, acc[q], 0.0)

    for k in range(tiles):
        node_ref[pl.ds(k, LANES, stride=tiles), 0:block] = jnp.transpose(
            x_ref[:, k * LANES : (k + 1) * LANES]
        )
    for t in range(tiles):
        out_ref[:, t * LANES : (t + 1) * LANES] = jnp.transpose(
            node_ref[t * LANES : (t + 1) * LANES, 0:block]
        )


def edge_kernel(
    far_ref, halo_ref, v_ref, up_ref, dn_ref, dc_ref, sr_ref, an_ref, sp_ref, sgn_ref, key_ref, mask_ref,
    acc_ref, old_ref, out_ref, price_ref, e_ref, p_ref,
):
    n, steps = v_ref.shape[0], up_ref.shape[0]
    i = pl.program_id(0)
    lane = lax.broadcasted_iota(jnp.int32, (ROWS, LANES), 1)

    @pl.when(i == 0)
    def _():
        far = far_ref[0]

        def joined(at, ref):
            mine = ref[...]
            beyond = halo_ref[n + at : n + at + mine.shape[0], :]
            here = lax.broadcasted_iota(jnp.int32, mine.shape, 1)
            return jnp.where(here < LANES // 2, beyond, mine)

        up, dn, dc, sr, an = (
            joined(j * steps, ref) for j, ref in enumerate((up_ref, dn_ref, dc_ref, sr_ref, an_ref))
        )
        price = jnp.where(lane < LANES // 2, halo_ref[n + 5 * steps : n + 5 * steps + ROWS, :], jnp.broadcast_to(sp_ref[sp_ref.shape[0] - 1 :, :], (ROWS, LANES)))
        price = jnp.where((lane < steps) | (lane >= LANES - steps), price, 0.0)
        a, b, c = scaled_rows(up, dn, dc, an)
        rim = lax.broadcasted_iota(jnp.int32, a.shape, 1)
        a = jnp.where((rim == LANES - 1) & (far == 1), 0.0, a)
        c = jnp.where((rim == 0) & (far == 1), 0.0, c)
        for half in range(2):
            at = [slice(half * LANES + q * ROWS, half * LANES + (q + 1) * ROWS) for q in range(LANES // ROWS)]
            x = [jnp.where(lane < LANES // 2, halo_ref[z, :], v_ref[z, :]) for z in at]
            sign, key, mask = ([ref[z, :] for z in at] for ref in (sgn_ref, key_ref, mask_ref))
            for s in range(steps):
                above = [pltpu.roll(z, LANES - 1, 1) for z in x]
                below = [pltpu.roll(z, 1, 1) for z in x]
                ra, rb, rc, rp = (jnp.broadcast_to(z[s : s + 1, :], (ROWS, LANES)) for z in (a, b, c, sr))
                for q in range(len(x)):
                    alpha, beta = on_terms(sign[q], key[q], mask[q], s)
                    x[q] = jnp.maximum(ra * above[q] + rb * x[q] + rc * below[q], alpha * rp - beta)
            fin = jnp.broadcast_to(an[steps - 1 : steps, :], (ROWS, LANES))
            for q, z in enumerate(at):
                e = x[q] * fin
                e_ref[z, :] = e
                p_ref[z, :] = acc_ref[z, :] + e * price
        for half in range(2):
            part = jnp.transpose(p_ref[half * LANES : (half + 1) * LANES, :])
            price_ref[half : half + 1, :] = jnp.sum(part, axis=0, keepdims=True)

    side = lax.broadcasted_iota(jnp.int32, (n, LANES), 1)

    @pl.when(i == 0)
    def _():
        out_ref[...] = jnp.where(side < steps, e_ref[...], old_ref[...])

    @pl.when(i == 1)
    def _():
        out_ref[...] = jnp.where(side >= LANES - steps, e_ref[...], old_ref[...])


def whole(shape):
    return pl.BlockSpec(shape, lambda i: (0,) * len(shape))


def vmem_scratch(shape):
    return pltpu.VMEM(shape, jnp.float32)


def local(values_in, prob_up, prob_down, discount, swap_rate, annuity, state_price, exercise_step, strike_bucket, notional_sign, strike_table):
    n, width = values_in.shape
    steps = prob_up.shape[0]
    node_count = lax.axis_size(NODE)
    tiles = width // LANES
    table = (prob_up, prob_down, discount, swap_rate, annuity)
    price_rows = state_price.reshape(tiles, LANES)
    trades = (exercise_step.T, strike_bucket.reshape(-1, LANES), notional_sign.reshape(-1, LANES), strike_table.reshape(1, -1))
    f32 = jnp.float32

    halo_rows = n + 5 * steps + ROWS
    packed = pl.pallas_call(
        pack_kernel,
        grid=(1,),
        in_specs=[whole((n, LANES))] + [whole((steps, LANES))] * 5 + [whole(price_rows.shape)],
        out_specs=whole((halo_rows, LANES)),
        out_shape=jax.ShapeDtypeStruct((halo_rows, LANES), f32),
        name="pack",
    )(values_in, *table, price_rows)
    halo = lax.ppermute(packed, NODE, [((i + 1) % node_count, i) for i in range(node_count)])

    block = LANES
    side = jax.ShapeDtypeStruct((n, LANES), f32)
    rolled, acc, sign, key, mask = pl.pallas_call(
        functools.partial(interior_kernel, 4),
        grid=(n // block,),
        in_specs=[pl.BlockSpec((block, width), lambda i: (i, 0))]
        + [whole((steps, width))] * 5
        + [whole(z.shape) for z in (price_rows,) + trades],
        out_specs=[
            pl.BlockSpec((block, width), lambda i: (i, 0)),
            pl.BlockSpec((block, LANES), lambda i: (i, 0)),
        ]
        + [whole((n, LANES))] * 3,
        out_shape=[jax.ShapeDtypeStruct((n, width), f32), side, side, side, jax.ShapeDtypeStruct((n, LANES), jnp.int32)],
        scratch_shapes=[
            vmem_scratch((LANES, width)),
            vmem_scratch((LANES, width)),
            vmem_scratch((block, width)),
            vmem_scratch((width, LANES)),
            vmem_scratch((2, 4 * ROWS, width)),
        ],
        cost_estimate=pl.CostEstimate(flops=12 * n * width * steps, bytes_accessed=3 * 8 * n * width, transcendentals=0),
        name="interior",
    )(values_in, *table, price_rows, *trades)

    far = (lax.axis_index(NODE) == node_count - 1).astype(jnp.int32).reshape(1)
    last_tile = lambda i: (0, tiles - 1)
    ends = pl.BlockSpec((n, LANES), lambda i: (0, i * (tiles - 1)))
    rolled, partial = pl.pallas_call(
        edge_kernel,
        grid=(2,),
        in_specs=[
            pl.BlockSpec(memory_space=pltpu.SMEM),
            whole((halo_rows, LANES)),
            pl.BlockSpec((n, LANES), last_tile),
        ]
        + [pl.BlockSpec((steps, LANES), last_tile)] * 5
        + [whole(price_rows.shape)]
        + [whole((n, LANES))] * 4
        + [ends],
        out_specs=[ends, whole((n // LANES, LANES))],
        out_shape=[jax.ShapeDtypeStruct((n, width), f32), jax.ShapeDtypeStruct((n // LANES, LANES), f32)],
        scratch_shapes=[vmem_scratch((n, LANES)), vmem_scratch((n, LANES))],
        input_output_aliases={13: 0},
        name="edge",
    )(far, halo, values_in, *table, price_rows, sign, key, mask, acc, rolled)

    rows = n // node_count
    moved = lax.all_to_all(rolled.reshape(node_count, rows, width), NODE, 0, 0, tiled=True)
    for axis in reversed(NODE):
        partial = lax.psum(partial, axis)
    mine = lax.dynamic_slice_in_dim(partial.reshape(node_count, rows), lax.axis_index(NODE), 1, 0)
    prices = mine.reshape(rows)
    total = jnp.sum(partial)
    for axis in reversed(TRADE):
        total = lax.psum(total, axis)

    flat = jnp.swapaxes(moved, 0, 1).reshape(rows, node_count * width)
    shifted = jnp.roll(flat, width, axis=1)
    column = lax.broadcasted_iota(jnp.int32, (1, node_count * width), 1)
    values = jnp.where(column % width < steps, shifted, flat)
    return values, prices, total / n


def solution(mesh):
    split = Mesh(mesh.devices.reshape(2, 2, 2, 2, 2, 2, 2), TRADE_NODE)
    in_specs = (
        P(TRADE, NODE),
        P(None, NODE),
        P(None, NODE),
        P(None, NODE),
        P(None, NODE),
        P(None, NODE),
        P(NODE),
        P(TRADE, None),
        P(TRADE),
        P(TRADE),
        P(),
    )
    out_specs = (P(TRADE_NODE, None), P(TRADE_NODE), P())
    return jax.shard_map(local, mesh=split, in_specs=in_specs, out_specs=out_specs, check_vma=False)
```

```python
import functools

import jax
import jax.numpy as jnp
from jax import lax
from jax.experimental import pallas as pl
from jax.experimental.pallas import tpu as pltpu
from jax.sharding import Mesh
from jax.sharding import PartitionSpec as P

LANES = 128
HALF = LANES // 2
ROWS = 8
CHUNKS = 2
TOGETHER = 4
OFF = 1e30
NODE = ("node_0", "node_1", "node_2")
TRADE_NODE = ("trade",) + NODE


def scaled_rows(up, down, disc, ann):
    row = lax.broadcasted_iota(jnp.int32, ann.shape, 0)
    width = ann.shape[1]
    before = jnp.where(row == 0, 1.0, pltpu.roll(ann, 1, 0))
    share = disc / ann
    a = share * up * pltpu.roll(before, width - 1, 1)
    b = share * (1.0 - up - down) * before
    c = share * down * pltpu.roll(before, 1, 1)
    return a, b, c


def trade_columns(ex_ref, bucket_ref, sign_ref, table_ref, half):
    ex = ex_ref[:, half * LANES : (half + 1) * LANES]
    bits = jnp.left_shift(jnp.ones_like(ex), ex)
    mask = bits[0:1] | bits[1:2] | bits[2:3] | bits[3:4]
    bucket = bucket_ref[half : half + 1, :]
    levels = lax.broadcasted_iota(jnp.int32, (table_ref.shape[1], LANES), 0)
    strike = jnp.dot(
        table_ref[...],
        (levels == bucket).astype(jnp.float32),
        precision=lax.Precision.HIGHEST,
        preferred_element_type=jnp.float32,
    )
    sign = (2 * sign_ref[half : half + 1, :] - 1).astype(jnp.float32)

    def column(r):
        return jnp.transpose(jnp.broadcast_to(r, (LANES, LANES)))

    return column(sign), column(sign * strike), column(mask.astype(jnp.float32)).astype(jnp.int32)


def on_terms(sign, key, mask, step):
    on = (mask & (1 << step)) != 0
    return jnp.where(on, sign, 0.0), jnp.where(on, key, OFF)


def pack_kernel(v_ref, up_ref, dn_ref, dc_ref, sr_ref, an_ref, sp_ref, out_ref):
    n, steps = v_ref.shape[0], up_ref.shape[0]
    out_ref[0:n, :] = v_ref[...]
    for i, ref in enumerate((up_ref, dn_ref, dc_ref, sr_ref, an_ref)):
        out_ref[n + i * steps : n + (i + 1) * steps, :] = ref[...]
    out_ref[n + 5 * steps : n + 5 * steps + ROWS, :] = jnp.broadcast_to(sp_ref[0:1, :], (ROWS, LANES))


def roll_kernel(
    last, far_ref, v_ref, up_ref, dn_ref, dc_ref, sr_ref, an_ref, sp_ref,
    v2_ref, up2_ref, dn2_ref, dc2_ref, sr2_ref, an2_ref, sp2_ref,
    ex_ref, bk_ref, sg_ref, tb_ref, *rest,
):
    if last:
        before_ref, out_ref, sum_ref = rest[:3]
    else:
        out_ref, sum_ref = rest[:2]
    nat_ref, coef_ref, strip_ref, x_ref, node_ref, buf_ref, rim_ref, e_ref, sgn_ref, key_ref, mask_ref = rest[2 + last :]
    steps, width = up_ref.shape
    tiles = width // LANES
    block = v_ref.shape[0]
    groups = block // ROWS
    spoiled = steps // tiles
    i = pl.program_id(0)
    lane = lax.broadcasted_iota(jnp.int32, (ROWS, LANES), 1)

    def cols(k):
        return slice(k * LANES, (k + 1) * LANES)

    def rows(q):
        return slice(q * ROWS, (q + 1) * ROWS)

    def spread(src, dst):
        for t in range(tiles):
            node_ref[cols(t), :] = jnp.transpose(src[:, cols(t)])
        for k in range(tiles):
            dst[:, cols(k)] = jnp.transpose(node_ref[pl.ds(k, LANES, stride=tiles), :])

    @pl.when(i == 0)
    def _():
        a, b, c = scaled_rows(up_ref[...], dn_ref[...], dc_ref[...], an_ref[...])
        for j, z in enumerate((a, b, c, sr_ref[...])):
            nat_ref[j * steps : (j + 1) * steps, :] = z
        nat_ref[4 * steps : 4 * steps + ROWS, :] = an_ref[steps - ROWS : steps, :]
        for t in range(tiles):
            nat_ref[4 * steps + ROWS : 4 * steps + 2 * ROWS, cols(t)] = jnp.broadcast_to(
                sp_ref[t : t + 1, :], (ROWS, LANES)
            )
        nat_ref[4 * steps + 2 * ROWS :, :] = jnp.zeros((LANES - 4 * steps - 2 * ROWS, width), jnp.float32)
        spread(nat_ref, coef_ref)

        side = lax.broadcasted_iota(jnp.int32, (steps, LANES), 1)

        def joined(ref, beyond):
            return jnp.where(side < HALF, beyond[...], ref[:, width - LANES :])

        an = joined(an_ref, an2_ref)
        a, b, c = scaled_rows(joined(up_ref, up2_ref), joined(dn_ref, dn2_ref), joined(dc_ref, dc2_ref), an)
        far = far_ref[0] == 1
        a = jnp.where((side == LANES - 1) & far, 0.0, a)
        c = jnp.where((side == 0) & far, 0.0, c)
        for j, z in enumerate((a, b, c, joined(sr_ref, sr2_ref))):
            strip_ref[j * steps : (j + 1) * steps, :] = z
        strip_ref[4 * steps : 4 * steps + ROWS, :] = an[steps - ROWS : steps, :]
        price = jnp.where(lane < HALF, sp2_ref[0:1, :], sp_ref[tiles - 1 : tiles, :])
        strip_ref[4 * steps + ROWS : 4 * steps + 2 * ROWS, :] = jnp.where(
            (lane < steps) | (lane >= LANES - steps), price, 0.0
        )
        for half in range(sgn_ref.shape[0] // LANES):
            sign, key, mask = trade_columns(ex_ref, bk_ref, sg_ref, tb_ref, half)
            at = pl.ds(half * LANES, LANES)
            sgn_ref[at, :] = sign
            key_ref[at, :] = key
            mask_ref[at, :] = mask
        if last:
            sum_ref[...] = jnp.zeros((ROWS, LANES), jnp.float32)

    spread(v_ref, x_ref)
    base = [pl.ds(pl.multiple_of(i * block + ROWS * q, ROWS), ROWS) for q in range(groups)]

    def wide(ref, r, at):
        return jnp.broadcast_to(ref[r : r + 1, at], (ROWS, LANES))

    def load(s, q, k):
        return x_ref[rows(q), cols(k)] if s == 0 else buf_ref[(s - 1) % 2, rows(q), cols(k)]

    def put_rim(s, q, first, final):
        rim_ref[s % 2, 0, rows(q), :] = pltpu.roll(first, LANES - 1, 1)
        rim_ref[s % 2, 1, rows(q), :] = pltpu.roll(final, 1, 1)

    def put_strip(s, q, e):
        e_ref[s % 2, 0, rows(q), :] = e
        e_ref[s % 2, 1, rows(q), :] = pltpu.roll(e, LANES - 1, 1)
        e_ref[s % 2, 2, rows(q), :] = pltpu.roll(e, 1, 1)

    for q in range(groups):
        put_rim(1, q, load(0, q, 0), load(0, q, tiles - 1))
        put_strip(1, q, jnp.where(lane < HALF, v2_ref[rows(q), :], v_ref[rows(q), width - LANES :]))
    acc = [None] * groups
    for s in range(steps):
        done = s == steps - 1
        for q0 in range(0, groups, TOGETHER):
            qs = range(q0, q0 + TOGETHER)
            terms = {q: on_terms(sgn_ref[base[q], :], key_ref[base[q], :], mask_ref[base[q], :], s) for q in qs}
            a, b, c, p = (wide(strip_ref, j * steps + s, slice(None)) for j in range(4))
            for q in qs:
                alpha, beta = terms[q]
                z = (s + 1) % 2
                e = a * e_ref[z, 1, rows(q), :] + b * e_ref[z, 0, rows(q), :] + c * e_ref[z, 2, rows(q), :]
                e = jnp.maximum(e, alpha * p - beta)
                if done:
                    e = e * strip_ref[4 * steps + ROWS - 1 : 4 * steps + ROWS, :]
                    e_ref[s % 2, 0, rows(q), :] = e
                    acc[q] = e * strip_ref[4 * steps + ROWS : 4 * steps + 2 * ROWS, :]
                else:
                    put_strip(s, q, e)
            below = {q: rim_ref[(s + 1) % 2, 1, rows(q), :] for q in qs}
            here = {q: load(s, q, 0) for q in qs}
            inner = {q: None for q in qs}
            first = {}
            for k in range(tiles):
                a, b, c, p = (wide(coef_ref, j * steps + s, cols(k)) for j in range(4))
                if done:
                    fin = wide(coef_ref, 4 * steps + ROWS - 1, cols(k))
                    price = wide(coef_ref, 4 * steps + ROWS, cols(k))
                for q in qs:
                    above = load(s, q, k + 1) if k + 1 < tiles else rim_ref[(s + 1) % 2, 0, rows(q), :]
                    alpha, beta = terms[q]
                    new = jnp.maximum(a * above + b * here[q] + c * below[q], alpha * p - beta)
                    below[q], here[q] = here[q], above
                    if done:
                        new = new * fin
                        x_ref[rows(q), cols(k)] = new
                        inner[q] = new * price if k == 0 else inner[q] + new * price
                    else:
                        buf_ref[s % 2, rows(q), cols(k)] = new
                        if k == 0:
                            first[q] = new
                        if k == tiles - 1:
                            put_rim(s, q, first[q], new)
            if done:
                for q in qs:
                    acc[q] = acc[q] + jnp.where((lane >= spoiled) & (lane < LANES - spoiled), inner[q], 0.0)

    for k in range(tiles):
        node_ref[pl.ds(k, LANES, stride=tiles), :] = jnp.transpose(x_ref[:, cols(k)])
    side = lax.broadcasted_iota(jnp.int32, (block, LANES), 1)
    strip = e_ref[(steps - 1) % 2, 0]
    for t in range(tiles):
        z = jnp.transpose(node_ref[cols(t), :])
        if t == 0:
            z = jnp.where(side < steps, strip, z)
        if t == tiles - 1:
            z = jnp.where(side >= LANES - steps, strip, z)
        out_ref[:, cols(t)] = z
    if last:
        total = sum_ref[...]
        for q in range(groups):
            both = acc[q] + before_ref[rows(q), :]
            out_ref[rows(q), cols(tiles)] = both + pltpu.roll(both, HALF, 1)
            total = total + both
        sum_ref[...] = total
    else:
        for q in range(groups):
            sum_ref[rows(q), :] = acc[q]


def finish_kernel(sources, steps, share, a_ref, b_ref, a0_ref, b0_ref, p_ref, out_ref, price_ref, total_ref):
    width = a_ref.shape[2]
    per = a_ref.shape[0]
    i = pl.program_id(0)
    lane = lax.broadcasted_iota(jnp.int32, (ROWS, LANES), 1)
    for j in range(per):
        left = lax.rem(i * per + j + sources - 1, sources)
        for h, ref in enumerate((a_ref, b_ref)):
            at = (2 * j + h) * width
            head = b0_ref[left] if h == 0 else a0_ref[i * per + j]
            out_ref[:, at : at + LANES] = jnp.where(lane < steps, head, ref[j, :, 0:LANES])
            out_ref[:, at + LANES : at + width] = ref[j, :, LANES:width]

    @pl.when(i == 0)
    def _():
        both = p_ref[0]
        for j in range(1, sources):
            both = both + p_ref[j]
        total_ref[0] = jnp.sum(jnp.where(lane >= HALF, both, 0.0)) / share
        mine = jnp.where(lane < HALF, both, 0.0)
        for r in range(ROWS):
            price_ref[r] = jnp.sum(mine[r : r + 1, :])


def whole(shape, index=None):
    at = index if index is not None else (0,) * len(shape)
    return pl.BlockSpec(shape, lambda i: at)


def vmem(*shape):
    return pltpu.VMEM(shape, jnp.float32)


def roll_chunk(h, far, values_in, table, price_rows, beyond, beyond_specs, trades, before):
    n, total_width = values_in.shape
    steps = table[0].shape[0]
    width = total_width // CHUNKS
    tiles = width // LANES
    block = LANES
    last = h == CHUNKS - 1
    out_width = width + LANES if last else width
    f32 = jnp.float32
    row_block = pl.BlockSpec((block, LANES), lambda i: (i, 0))
    return pl.pallas_call(
        functools.partial(roll_kernel, last),
        grid=(n // block,),
        in_specs=[pl.BlockSpec(memory_space=pltpu.SMEM), pl.BlockSpec((block, width), lambda i: (i, h))]
        + [whole((steps, width), (0, h))] * 5
        + [whole((tiles, LANES), (h, 0))]
        + beyond_specs
        + [whole(z.shape) for z in trades]
        + ([row_block] if last else []),
        out_specs=[
            pl.BlockSpec((block, out_width), lambda i: (i, 0)),
            whole((ROWS, LANES)) if last else row_block,
        ],
        out_shape=[
            jax.ShapeDtypeStruct((n, out_width), f32),
            jax.ShapeDtypeStruct((ROWS, LANES) if last else (n, LANES), f32),
        ],
        scratch_shapes=[
            vmem(LANES, width),
            vmem(LANES, width),
            vmem(LANES, LANES),
            vmem(block, width),
            vmem(width, LANES),
            vmem(2, block, width),
            vmem(2, 2, block, LANES),
            vmem(2, 3, block, LANES),
            vmem(n, LANES),
            vmem(n, LANES),
            pltpu.VMEM((n, LANES), jnp.int32),
        ],
        cost_estimate=pl.CostEstimate(
            flops=12 * n * width * steps, bytes_accessed=3 * 4 * n * width, transcendentals=0
        ),
        name="roll_last" if last else "roll_first",
    )(far, values_in, *table, price_rows, *beyond, *trades, *before)


def local(values_in, prob_up, prob_down, discount, swap_rate, annuity, state_price, exercise_step, strike_bucket, notional_sign, strike_table):
    n, total_width = values_in.shape
    steps = prob_up.shape[0]
    node_count = lax.axis_size(NODE)
    trade_count = lax.axis_size("trade")
    width = total_width // CHUNKS
    tiles = width // LANES
    table = (prob_up, prob_down, discount, swap_rate, annuity)
    price_rows = state_price.reshape(-1, LANES)
    trades = (exercise_step.T, strike_bucket.reshape(-1, LANES), notional_sign.reshape(-1, LANES), strike_table.reshape(1, -1))
    f32 = jnp.float32
    block = LANES

    halo_rows = n + 5 * steps + ROWS
    packed = pl.pallas_call(
        pack_kernel,
        grid=(1,),
        in_specs=[whole((n, LANES))] + [whole((steps, LANES))] * 5 + [whole(price_rows.shape)],
        out_specs=whole((halo_rows, LANES)),
        out_shape=jax.ShapeDtypeStruct((halo_rows, LANES), f32),
        name="pack",
    )(values_in, *table, price_rows)
    halo = lax.ppermute(packed, NODE, [((i + 1) % node_count, i) for i in range(node_count)])
    far = (lax.axis_index(NODE) == node_count - 1).astype(jnp.int32).reshape(1)

    inner_specs = (
        [pl.BlockSpec((block, LANES), lambda i: (i, tiles))]
        + [whole((steps, LANES), (0, tiles))] * 5
        + [whole((tiles, LANES), (1, 0))]
    )
    first, first_sums = roll_chunk(
        0, jnp.zeros((1,), jnp.int32), values_in, table, price_rows,
        (values_in,) + table + (price_rows,), inner_specs, trades, (),
    )
    halo_specs = (
        [pl.BlockSpec((block, LANES), lambda i: (i, 0))]
        + [whole((steps, LANES), (n // steps + j, 0)) for j in range(5)]
        + [whole((ROWS, LANES), ((n + 5 * steps) // ROWS, 0))]
    )
    rows = n // node_count
    first_moved = lax.all_to_all(first.reshape(node_count, rows, width), NODE, 0, 0, tiled=True)
    second, sums = roll_chunk(
        1, far, values_in, table, price_rows, (halo,) * 7, halo_specs, trades, (first_sums,)
    )
    total = sums
    for k in range(1, trade_count):
        total = total + lax.ppermute(sums, "trade", [(i, (i + k) % trade_count) for i in range(trade_count)])
    total = total + jnp.roll(total, HALF, axis=1)
    lane = lax.broadcasted_iota(jnp.int32, (node_count, rows, LANES), 2)
    blocks = second.reshape(node_count, rows, width + LANES)
    tail = jnp.where(lane < HALF, blocks[:, :, width:], total[None])
    blocks = lax.dynamic_update_slice_in_dim(blocks, tail, width, 2)
    second_moved = lax.all_to_all(blocks, NODE, 0, 0, tiled=True)

    per = 4
    values, prices, portfolio = pl.pallas_call(
        functools.partial(finish_kernel, node_count, steps, float(n)),
        grid=(node_count // per,),
        in_specs=[
            pl.BlockSpec((per, rows, width), lambda i: (i, 0, 0)),
            pl.BlockSpec((per, rows, width), lambda i: (i, 0, 0)),
            whole((node_count, rows, LANES)),
            whole((node_count, rows, LANES)),
            whole((node_count, rows, LANES), (0, 0, tiles)),
        ],
        out_specs=[
            pl.BlockSpec((rows, per * total_width), lambda i: (0, i)),
            pl.BlockSpec(memory_space=pltpu.SMEM),
            pl.BlockSpec(memory_space=pltpu.SMEM),
        ],
        out_shape=[
            jax.ShapeDtypeStruct((rows, node_count * total_width), f32),
            jax.ShapeDtypeStruct((rows,), f32),
            jax.ShapeDtypeStruct((1,), f32),
        ],
        name="finish",
    )(first_moved, second_moved, first_moved, second_moved, second_moved)
    return values, prices, portfolio.reshape(())


def solution(mesh):
    split = Mesh(mesh.devices.reshape(mesh.shape["trade"], 4, 4, 2), TRADE_NODE)
    in_specs = (
        P("trade", NODE),
        P(None, NODE),
        P(None, NODE),
        P(None, NODE),
        P(None, NODE),
        P(None, NODE),
        P(NODE),
        P("trade", None),
        P("trade"),
        P("trade"),
        P(),
    )
    out_specs = (P(TRADE_NODE, None), P(TRADE_NODE), P())
    return jax.shard_map(local, mesh=split, in_specs=in_specs, out_specs=out_specs, check_vma=False)
```

```python
import functools

import jax
import jax.numpy as jnp
from jax import lax
from jax.experimental import pallas as pl
from jax.experimental.pallas import tpu as pltpu
from jax.sharding import Mesh
from jax.sharding import PartitionSpec as P

LANES = 128
HALF = LANES // 2
ROWS = 8
FIRST_TILES = 10
TOGETHER = 4
OFF = 1e30
NODE = ("node_0", "node_1", "node_2")
TRADE_NODE = ("trade",) + NODE


def scaled_rows(up, down, disc, ann):
    row = lax.broadcasted_iota(jnp.int32, ann.shape, 0)
    width = ann.shape[1]
    before = jnp.where(row == 0, 1.0, pltpu.roll(ann, 1, 0))
    share = disc / ann
    a = share * up * pltpu.roll(before, width - 1, 1)
    b = share * (1.0 - up - down) * before
    c = share * down * pltpu.roll(before, 1, 1)
    return a, b, c


def trade_columns(ex_ref, bucket_ref, sign_ref, table_ref, half):
    ex = ex_ref[:, half * LANES : (half + 1) * LANES]
    bits = jnp.left_shift(jnp.ones_like(ex), ex)
    mask = bits[0:1] | bits[1:2] | bits[2:3] | bits[3:4]
    bucket = bucket_ref[half : half + 1, :]
    levels = lax.broadcasted_iota(jnp.int32, (table_ref.shape[1], LANES), 0)
    strike = jnp.dot(
        table_ref[...],
        (levels == bucket).astype(jnp.float32),
        precision=lax.Precision.HIGHEST,
        preferred_element_type=jnp.float32,
    )
    sign = (2 * sign_ref[half : half + 1, :] - 1).astype(jnp.float32)

    def column(r):
        return jnp.transpose(jnp.broadcast_to(r, (LANES, LANES)))

    return column(sign), column(sign * strike), column(mask.astype(jnp.float32)).astype(jnp.int32)


def on_terms(sign, key, mask, step):
    on = (mask & (1 << step)) != 0
    return jnp.where(on, sign, 0.0), jnp.where(on, key, OFF)


def roll_kernel(start, last, far_ref, v_ref, up_ref, dn_ref, dc_ref, sr_ref, an_ref, *rest):
    smalls, rest = rest[:5], rest[5:]
    if last:
        halo_ref, before_ref, out_ref, price_ref, sum_ref = rest[:5]
    else:
        out_ref, sum_ref, pack_ref, pack_sems = rest[0], rest[1], rest[2], rest[-1]
        rest = rest[:-1]
    (
        nat_ref, coef_ref, strip_ref, x_ref, node_ref, buf_ref, rim_ref, e_ref, sgn_ref, key_ref, mask_ref,
        own_ref, table_ref, stage_ref, table_sems, own_sems, out_sems,
        sp_ref, ex_ref, bk_ref, sg_ref, tb_ref, small_sems,
    ) = rest[-23:]
    n, steps = v_ref.shape[0], up_ref.shape[0]
    width = x_ref.shape[1]
    stop = start + width
    tiles = width // LANES
    block = x_ref.shape[0]
    groups = block // ROWS
    lane = lax.broadcasted_iota(jnp.int32, (ROWS, LANES), 1)

    def cols(k):
        return slice(k * LANES, (k + 1) * LANES)

    def rows(q):
        return slice(q * ROWS, (q + 1) * ROWS)

    def spread(src, dst):
        for t in range(tiles):
            node_ref[cols(t), :] = jnp.transpose(src(t))
        for k in range(tiles):
            dst[:, cols(k)] = jnp.transpose(node_ref[pl.ds(k, LANES, stride=tiles), :])

    seen = own_ref.shape[1]
    from_start = pl.ds(start, seen)
    table_copies = [
        pltpu.make_async_copy(ref.at[:, from_start], table_ref.at[j], table_sems.at[j])
        for j, ref in enumerate((up_ref, dn_ref, dc_ref, sr_ref, an_ref))
    ]
    own_copies = [
        pltpu.make_async_copy(
            v_ref.at[pl.ds(i * block, block), from_start], own_ref.at[pl.ds(i * block, block), :], own_sems.at[i]
        )
        for i in range(n // block)
    ]
    small_copies = [
        pltpu.make_async_copy(src, dst, small_sems.at[j])
        for j, (src, dst) in enumerate(zip(smalls, (sp_ref, ex_ref, bk_ref, sg_ref, tb_ref)))
    ]
    for copy in small_copies + table_copies + own_copies:
        copy.start()
    for copy in small_copies:
        copy.wait()
    for half in range(n // LANES):
        sign, key, mask = trade_columns(ex_ref, bk_ref, sg_ref, tb_ref, half)
        at = pl.ds(half * LANES, LANES)
        sgn_ref[at, :] = sign
        key_ref[at, :] = key
        mask_ref[at, :] = mask
    if last:
        sum_ref[...] = jnp.zeros((ROWS, LANES), jnp.float32)
    for copy in table_copies:
        copy.wait()
    pack_copies = []
    if not last:
        tile = pl.ds(0, LANES)
        pack_copies = [
            pltpu.make_async_copy(table_ref.at[j, :, tile], pack_ref.at[pl.ds(n + j * steps, steps), :], pack_sems.at[j])
            for j in range(5)
        ]
        pack_copies.append(
            pltpu.make_async_copy(
                sp_ref.at[pl.ds(0, ROWS), :], pack_ref.at[pl.ds(n + 5 * steps, ROWS), :], pack_sems.at[5]
            )
        )
        for copy in pack_copies:
            copy.start()

    up, dn, dc, sr, an = (table_ref[j, :, 0:width] for j in range(5))
    a, b, c = scaled_rows(up, dn, dc, an)
    for j, z in enumerate((a, b, c, sr)):
        nat_ref[j * steps : (j + 1) * steps, :] = z
    nat_ref[4 * steps : 4 * steps + ROWS, :] = an[steps - ROWS : steps, :]
    for t in range(tiles):
        price = sp_ref[start // LANES + t : start // LANES + t + 1, :]
        if t == 0:
            price = jnp.where(lane < steps, 0.0, price)
        if t == tiles - 1:
            price = jnp.where(lane >= LANES - steps, 0.0, price)
        nat_ref[4 * steps + ROWS : 4 * steps + 2 * ROWS, cols(t)] = jnp.broadcast_to(price, (ROWS, LANES))
    nat_ref[4 * steps + 2 * ROWS :, :] = jnp.zeros((LANES - 4 * steps - 2 * ROWS, width), jnp.float32)
    spread(lambda t: nat_ref[:, cols(t)], coef_ref)

    side = lax.broadcasted_iota(jnp.int32, (steps, LANES), 1)

    def joined(j):
        beyond = halo_ref[n + j * steps : n + (j + 1) * steps, :] if last else table_ref[j, :, width:seen]
        return jnp.where(side < HALF, beyond, table_ref[j, :, width - LANES : width])

    strip_an = joined(4)
    a, b, c = scaled_rows(joined(0), joined(1), joined(2), strip_an)
    if last:
        far = far_ref[0] == 1
        a = jnp.where((side == LANES - 1) & far, 0.0, a)
        c = jnp.where((side == 0) & far, 0.0, c)
    for j, z in enumerate((a, b, c, joined(3))):
        strip_ref[j * steps : (j + 1) * steps, :] = z
    strip_ref[4 * steps : 4 * steps + ROWS, :] = strip_an[steps - ROWS : steps, :]
    beyond = halo_ref[n + 5 * steps : n + 5 * steps + 1, :] if last else sp_ref[stop // LANES : stop // LANES + 1, :]
    price = jnp.where(lane < HALF, beyond, sp_ref[stop // LANES - 1 : stop // LANES, :])
    strip_ref[4 * steps + ROWS : 4 * steps + 2 * ROWS, :] = jnp.where(
        (lane < steps) | (lane >= LANES - steps), price, 0.0
    )

    def wide(ref, r, at):
        return jnp.broadcast_to(ref[r : r + 1, at], (ROWS, LANES))

    def load(s, q, k):
        return x_ref[rows(q), cols(k)] if s == 0 else buf_ref[(s - 1) % 2, rows(q), cols(k)]

    def put_rim(s, q, first, final):
        rim_ref[s % 2, 0, rows(q), :] = pltpu.roll(first, LANES - 1, 1)
        rim_ref[s % 2, 1, rows(q), :] = pltpu.roll(final, 1, 1)

    def put_strip(s, q, e):
        e_ref[s % 2, 0, rows(q), :] = e
        e_ref[s % 2, 1, rows(q), :] = pltpu.roll(e, LANES - 1, 1)
        e_ref[s % 2, 2, rows(q), :] = pltpu.roll(e, 1, 1)

    @pl.loop(0, n // block)
    def _(i):
        all_rows = pl.ds(pl.multiple_of(i * block, block), block)
        base = [pl.ds(pl.multiple_of(i * block + ROWS * q, ROWS), ROWS) for q in range(groups)]
        pltpu.make_async_copy(
            v_ref.at[all_rows, from_start], own_ref.at[all_rows, :], own_sems.at[i]
        ).wait()
        if not last:
            pltpu.make_async_copy(
                own_ref.at[all_rows, pl.ds(0, LANES)], pack_ref.at[all_rows, :], pack_sems.at[6 + i]
            ).start()
        spread(lambda t: own_ref[all_rows, cols(t)], x_ref)
        for q in range(groups):
            put_rim(1, q, load(0, q, 0), load(0, q, tiles - 1))
            beyond = halo_ref[base[q], :] if last else own_ref[base[q], width:seen]
            put_strip(1, q, jnp.where(lane < HALF, beyond, own_ref[base[q], width - LANES : width]))
        acc = [None] * groups
        for s in range(steps):
            done = s == steps - 1
            for q0 in range(0, groups, TOGETHER):
                qs = range(q0, q0 + TOGETHER)
                terms = {q: on_terms(sgn_ref[base[q], :], key_ref[base[q], :], mask_ref[base[q], :], s) for q in qs}
                a, b, c, p = (wide(strip_ref, j * steps + s, slice(None)) for j in range(4))
                for q in qs:
                    alpha, beta = terms[q]
                    z = (s + 1) % 2
                    e = a * e_ref[z, 1, rows(q), :] + b * e_ref[z, 0, rows(q), :] + c * e_ref[z, 2, rows(q), :]
                    e = jnp.maximum(e, alpha * p - beta)
                    if done:
                        e = e * strip_ref[4 * steps + ROWS - 1 : 4 * steps + ROWS, :]
                        e_ref[s % 2, 0, rows(q), :] = e
                        acc[q] = e * strip_ref[4 * steps + ROWS : 4 * steps + 2 * ROWS, :]
                    else:
                        put_strip(s, q, e)
                below = {q: rim_ref[(s + 1) % 2, 1, rows(q), :] for q in qs}
                here = {q: load(s, q, 0) for q in qs}
                first = {}
                for k in range(tiles):
                    a, b, c, p = (wide(coef_ref, j * steps + s, cols(k)) for j in range(4))
                    if done:
                        fin = wide(coef_ref, 4 * steps + ROWS - 1, cols(k))
                        price = wide(coef_ref, 4 * steps + ROWS, cols(k))
                    for q in qs:
                        above = load(s, q, k + 1) if k + 1 < tiles else rim_ref[(s + 1) % 2, 0, rows(q), :]
                        alpha, beta = terms[q]
                        new = jnp.maximum(a * above + b * here[q] + c * below[q], alpha * p - beta)
                        below[q], here[q] = here[q], above
                        if done:
                            new = new * fin
                            x_ref[rows(q), cols(k)] = new
                            acc[q] = acc[q] + new * price
                        else:
                            buf_ref[s % 2, rows(q), cols(k)] = new
                            if k == 0:
                                first[q] = new
                            if k == tiles - 1:
                                put_rim(s, q, first[q], new)

        for k in range(tiles):
            node_ref[pl.ds(k, LANES, stride=tiles), :] = jnp.transpose(x_ref[:, cols(k)])
        rim = lax.broadcasted_iota(jnp.int32, (block, LANES), 1)
        strip = e_ref[(steps - 1) % 2, 0]
        for t in range(tiles):
            z = jnp.transpose(node_ref[cols(t), :])
            if t == 0:
                z = jnp.where(rim < steps, strip, z)
            if t == tiles - 1:
                z = jnp.where(rim >= LANES - steps, strip, z)
            stage_ref[all_rows, cols(t)] = z
            here = pl.ds(t * LANES, LANES)
            pltpu.make_async_copy(stage_ref.at[all_rows, here], out_ref.at[all_rows, here], out_sems.at[i, t]).start()
        if last:
            total = sum_ref[...]
            for q in range(groups):
                both = acc[q] + before_ref[base[q], :]
                price_ref[base[q], :] = both + pltpu.roll(both, HALF, 1)
                total = total + both
            sum_ref[...] = total
        else:
            for q in range(groups):
                sum_ref[base[q], :] = acc[q]

    for i in range(n // block):
        at = pl.ds(i * block, block)
        for t in range(tiles):
            tile = pl.ds(t * LANES, LANES)
            pltpu.make_async_copy(stage_ref.at[at, tile], out_ref.at[at, tile], out_sems.at[i, t]).wait()
        if not last:
            pltpu.make_async_copy(
                own_ref.at[at, pl.ds(0, LANES)], pack_ref.at[at, :], pack_sems.at[6 + i]
            ).wait()
    for copy in pack_copies:
        copy.wait()


def tail_kernel(sum_ref, *refs):
    *moved, price_ref, old_ref, out_ref, tail_ref, sem = refs
    del old_ref
    total = sum_ref[...]
    for ref in moved:
        total = total + ref[...]
    total = total + pltpu.roll(total, HALF, 1)
    lane = lax.broadcasted_iota(jnp.int32, (ROWS, LANES), 1)
    for q in range(tail_ref.shape[0] // ROWS):
        rows = slice(q * ROWS, (q + 1) * ROWS)
        tail_ref[rows, :] = jnp.where(lane < HALF, price_ref[rows, :], total)
    copy = pltpu.make_async_copy(tail_ref, out_ref.at[:, pl.ds(out_ref.shape[1] - LANES, LANES)], sem)
    copy.start()
    copy.wait()


def first_half_kernel(sources, total_width, a_ref, out_ref, sems):
    width = a_ref.shape[2]
    copies = [
        pltpu.make_async_copy(
            a_ref.at[j, :, pl.ds(LANES, width - LANES)],
            out_ref.at[:, pl.ds(j * total_width + LANES, width - LANES)],
            sems.at[j],
        )
        for j in range(sources)
    ]
    for copy in copies:
        copy.start()
    for copy in copies:
        copy.wait()


def second_half_kernel(
    sources, total_width, steps, share, a_ref, b_ref, old_ref, out_ref, price_ref, total_ref, head_ref, body_ref, sems
):
    del old_ref
    width = total_width - a_ref.shape[2]
    lane = lax.broadcasted_iota(jnp.int32, (ROWS, LANES), 1)
    copies = []
    for j in range(sources):
        left = (j + sources - 1) % sources
        at = slice(j * width, j * width + LANES)
        head_ref[:, j * LANES : (j + 1) * LANES] = jnp.where(
            lane < steps, b_ref[left, :, 0:LANES], a_ref[j, :, 0:LANES]
        )
        body_ref[:, at] = jnp.where(lane < steps, a_ref[j, :, 0:LANES], b_ref[j, :, 0:LANES])
        body_ref[:, j * width + LANES : (j + 1) * width] = b_ref[j, :, LANES:width]
        copies.append(
            pltpu.make_async_copy(
                head_ref.at[:, pl.ds(j * LANES, LANES)],
                out_ref.at[:, pl.ds(j * total_width, LANES)],
                sems.at[0, j],
            )
        )
        copies.append(
            pltpu.make_async_copy(
                body_ref.at[:, pl.ds(j * width, width)],
                out_ref.at[:, pl.ds((j + 1) * total_width - width, width)],
                sems.at[1, j],
            )
        )
        copies[-2].start()
        copies[-1].start()
    both = b_ref[0, :, width:]
    for j in range(1, sources):
        both = both + b_ref[j, :, width:]
    total_ref[0] = jnp.sum(jnp.where(lane >= HALF, both, 0.0)) / share
    mine = jnp.where(lane < HALF, both, 0.0)
    for r in range(ROWS):
        price_ref[r] = jnp.sum(mine[r : r + 1, :])
    for copy in copies:
        copy.wait()


def vmem(*shape):
    return pltpu.VMEM(shape, jnp.float32)


HERE = pl.BlockSpec(memory_space=pltpu.VMEM)
SCALARS = pl.BlockSpec(memory_space=pltpu.SMEM)
FAR = pl.BlockSpec(memory_space=pltpu.HBM)


def here(x):
    return pltpu.with_memory_space_constraint(x, pltpu.VMEM)


def roll_chunk(start, width, far, arrays, extra):
    n, total_width = arrays[0].shape
    steps = arrays[1].shape[0]
    last = start + width == total_width
    out_width = width + LANES if last else width
    seen = width if last else width + LANES
    f32 = jnp.float32
    return pl.pallas_call(
        functools.partial(roll_kernel, start, last),
        in_specs=[SCALARS] + [FAR] * len(arrays) + [HERE] * len(extra),
        out_specs=[FAR, HERE, HERE if last else FAR],
        out_shape=[
            jax.ShapeDtypeStruct((n, out_width), f32),
            jax.ShapeDtypeStruct((n, LANES), f32),
            jax.ShapeDtypeStruct((ROWS if last else n + 5 * steps + ROWS, LANES), f32),
        ],
        scratch_shapes=[
            vmem(LANES, width),
            vmem(LANES, width),
            vmem(LANES, LANES),
            vmem(LANES, width),
            vmem(width, LANES),
            vmem(2, LANES, width),
            vmem(2, 2, LANES, LANES),
            vmem(2, 3, LANES, LANES),
            vmem(n, LANES),
            vmem(n, LANES),
            pltpu.VMEM((n, LANES), jnp.int32),
            vmem(n, seen),
            vmem(5, steps, seen),
            vmem(n, width),
            pltpu.SemaphoreType.DMA((5,)),
            pltpu.SemaphoreType.DMA((n // LANES,)),
            pltpu.SemaphoreType.DMA((n // LANES, width // LANES)),
        ]
        + [pltpu.VMEM(z.shape, z.dtype) for z in arrays[6:]]
        + [pltpu.SemaphoreType.DMA((5,))]
        + ([] if last else [pltpu.SemaphoreType.DMA((6 + n // LANES,))]),
        cost_estimate=pl.CostEstimate(
            flops=12 * n * width * steps, bytes_accessed=3 * 4 * n * width, transcendentals=0
        ),
        name="roll_last" if last else "roll_first",
    )(far, *arrays, *extra)


def local(values_in, prob_up, prob_down, discount, swap_rate, annuity, state_price, exercise_step, strike_bucket, notional_sign, strike_table):
    n, total_width = values_in.shape
    steps = prob_up.shape[0]
    node_count = lax.axis_size(NODE)
    trade_count = lax.axis_size("trade")
    rows = n // node_count
    first_width = FIRST_TILES * LANES
    second_width = total_width - first_width
    f32 = jnp.float32
    table = (prob_up, prob_down, discount, swap_rate, annuity)
    price_rows = state_price.reshape(-1, LANES)
    trades = (exercise_step.T, strike_bucket.reshape(-1, LANES), notional_sign.reshape(-1, LANES), strike_table.reshape(1, -1))

    far = (lax.axis_index(NODE) == node_count - 1).astype(jnp.int32).reshape(1)

    arrays = (values_in,) + table + (price_rows,) + trades
    first, first_sums, packed = roll_chunk(0, first_width, jnp.zeros((1,), jnp.int32), arrays, ())
    halo = lax.ppermute(packed, NODE, [((i + 1) % node_count, i) for i in range(node_count)])
    first_moved = lax.all_to_all(first.reshape(node_count, rows, first_width), NODE, 0, 0, tiled=True)
    second, part, sums = roll_chunk(first_width, second_width, far, arrays, (here(halo), first_sums))
    moved_sums = [
        lax.ppermute(sums, "trade", [(i, (i + k) % trade_count) for i in range(trade_count)])
        for k in range(1, trade_count)
    ]
    second = pl.pallas_call(
        tail_kernel,
        in_specs=[HERE] * (trade_count + 1) + [FAR],
        out_specs=FAR,
        out_shape=jax.ShapeDtypeStruct(second.shape, f32),
        scratch_shapes=[vmem(n, LANES), pltpu.SemaphoreType.DMA(())],
        input_output_aliases={trade_count + 1: 0},
        name="tail",
    )(sums, *(here(z) for z in moved_sums), part, second)
    second_moved = lax.all_to_all(
        second.reshape(node_count, rows, second_width + LANES), NODE, 0, 0, tiled=True
    )

    out_shape = jax.ShapeDtypeStruct((rows, node_count * total_width), f32)
    half = pl.pallas_call(
        functools.partial(first_half_kernel, node_count, total_width),
        in_specs=[HERE],
        out_specs=FAR,
        out_shape=out_shape,
        scratch_shapes=[pltpu.SemaphoreType.DMA((node_count,))],
        cost_estimate=pl.CostEstimate(flops=4 * n * total_width, bytes_accessed=8 * n * first_width, transcendentals=0),
        name="first_half",
    )(here(first_moved))
    values, prices, portfolio = pl.pallas_call(
        functools.partial(second_half_kernel, node_count, total_width, steps, float(n)),
        in_specs=[HERE, HERE, FAR],
        out_specs=[FAR, SCALARS, SCALARS],
        out_shape=[out_shape, jax.ShapeDtypeStruct((rows,), f32), jax.ShapeDtypeStruct((1,), f32)],
        scratch_shapes=[
            vmem(rows, node_count * LANES),
            vmem(rows, node_count * second_width),
            pltpu.SemaphoreType.DMA((2, node_count)),
        ],
        input_output_aliases={2: 0},
        name="second_half",
    )(here(first_moved), here(second_moved), half)
    return values, prices, portfolio.reshape(())


def solution(mesh):
    split = Mesh(mesh.devices.reshape(mesh.shape["trade"], 4, 4, 2), TRADE_NODE)
    in_specs = (
        P("trade", NODE),
        P(None, NODE),
        P(None, NODE),
        P(None, NODE),
        P(None, NODE),
        P(None, NODE),
        P(NODE),
        P("trade", None),
        P("trade"),
        P("trade"),
        P(),
    )
    out_specs = (P(TRADE_NODE, None), P(TRADE_NODE), P())

    return jax.shard_map(local, mesh=split, in_specs=in_specs, out_specs=out_specs, check_vma=False)
```

```python
import functools

import jax
import jax.numpy as jnp
from jax import lax
from jax.experimental import pallas as pl
from jax.experimental.pallas import tpu as pltpu
from jax.sharding import Mesh
from jax.sharding import PartitionSpec as P

LANES = 128
HALF = LANES // 2
ROWS = 8
FIRST_TILES = 10
TOGETHER = 16
OFF = 1e30
NODE = ("node_0", "node_1", "node_2")
TRADE_NODE = ("trade",) + NODE


def scaled_rows(up, down, disc, ann):
    row = lax.broadcasted_iota(jnp.int32, ann.shape, 0)
    width = ann.shape[1]
    before = jnp.where(row == 0, 1.0, pltpu.roll(ann, 1, 0))
    share = disc / ann
    a = share * up * pltpu.roll(before, width - 1, 1)
    b = share * (1.0 - up - down) * before
    c = share * down * pltpu.roll(before, 1, 1)
    return a, b, c


def trade_columns(ex_ref, bucket_ref, sign_ref, table_ref, half):
    ex = ex_ref[:, half * LANES : (half + 1) * LANES]
    bits = jnp.left_shift(jnp.ones_like(ex), ex)
    mask = bits[0:1] | bits[1:2] | bits[2:3] | bits[3:4]
    bucket = bucket_ref[half : half + 1, :]
    levels = lax.broadcasted_iota(jnp.int32, (table_ref.shape[1], LANES), 0)
    strike = jnp.dot(
        table_ref[...],
        (levels == bucket).astype(jnp.float32),
        precision=lax.Precision.HIGHEST,
        preferred_element_type=jnp.float32,
    )
    sign = (2 * sign_ref[half : half + 1, :] - 1).astype(jnp.float32)

    def column(r):
        return jnp.transpose(jnp.broadcast_to(r, (LANES, LANES)))

    return column(sign), column(sign * strike), column(mask.astype(jnp.float32)).astype(jnp.int32)


def on_terms(sign, key, mask, step):
    on = (mask & (1 << step)) != 0
    return jnp.where(on, sign, 0.0), jnp.where(on, key, OFF)


def roll_kernel(start, last, far_ref, v_ref, up_ref, dn_ref, dc_ref, sr_ref, an_ref, *rest):
    smalls, rest = rest[:5], rest[5:]
    if last:
        halo_ref, before_hbm, out_ref, price_hbm, sum_hbm = rest[:5]
        before_ref, total_ref, last_sems = rest[-3:]
        rest = rest[:-3]
    else:
        out_ref, price_hbm, pack_ref, pack_sems = rest[0], rest[1], rest[2], rest[-1]
        rest = rest[:-1]
    (
        nat_ref, coef_ref, strip_ref, x_ref, node_ref, buf_ref, rim_ref, e_ref, sgn_ref, key_ref, mask_ref,
        own_ref, table_ref, stage_ref, table_sems, own_sems, out_sems,
        sp_ref, ex_ref, bk_ref, sg_ref, tb_ref, small_sems, price_ref, price_sems,
    ) = rest[-25:]
    n, steps = v_ref.shape[0], up_ref.shape[0]
    width = x_ref.shape[1]
    stop = start + width
    tiles = width // LANES
    block = x_ref.shape[0]
    groups = block // ROWS
    lane = lax.broadcasted_iota(jnp.int32, (ROWS, LANES), 1)

    def cols(k):
        return slice(k * LANES, (k + 1) * LANES)

    def rows(q):
        return slice(q * ROWS, (q + 1) * ROWS)

    def spread(src, dst):
        for t in range(tiles):
            node_ref[cols(t), :] = jnp.transpose(src(t))
        for k in range(tiles):
            dst[:, cols(k)] = jnp.transpose(node_ref[pl.ds(k, LANES, stride=tiles), :])

    seen = own_ref.shape[1]
    from_start = pl.ds(start, seen)
    table_copies = [
        pltpu.make_async_copy(ref.at[:, from_start], table_ref.at[j], table_sems.at[j])
        for j, ref in enumerate((up_ref, dn_ref, dc_ref, sr_ref, an_ref))
    ]
    own_copies = [
        pltpu.make_async_copy(
            v_ref.at[pl.ds(i * block, block), from_start], own_ref.at[pl.ds(i * block, block), :], own_sems.at[i]
        )
        for i in range(n // block)
    ]
    small_copies = [
        pltpu.make_async_copy(src, dst, small_sems.at[j])
        for j, (src, dst) in enumerate(zip(smalls, (sp_ref, ex_ref, bk_ref, sg_ref, tb_ref)))
    ]
    for copy in small_copies + table_copies + own_copies:
        copy.start()
    if last:
        before_copy = pltpu.make_async_copy(before_hbm, before_ref, last_sems.at[0])
        before_copy.start()
    for copy in small_copies:
        copy.wait()
    for half in range(n // LANES):
        sign, key, mask = trade_columns(ex_ref, bk_ref, sg_ref, tb_ref, half)
        at = pl.ds(half * LANES, LANES)
        sgn_ref[at, :] = sign
        key_ref[at, :] = key
        mask_ref[at, :] = mask
    if last:
        total_ref[...] = jnp.zeros((ROWS, LANES), jnp.float32)
        before_copy.wait()
    for copy in table_copies:
        copy.wait()
    pack_copies = []
    if not last:
        tile = pl.ds(0, LANES)
        pack_copies = [
            pltpu.make_async_copy(table_ref.at[j, :, tile], pack_ref.at[pl.ds(n + j * steps, steps), :], pack_sems.at[j])
            for j in range(5)
        ]
        pack_copies.append(
            pltpu.make_async_copy(
                sp_ref.at[pl.ds(0, ROWS), :], pack_ref.at[pl.ds(n + 5 * steps, ROWS), :], pack_sems.at[5]
            )
        )
        for copy in pack_copies:
            copy.start()

    up, dn, dc, sr, an = (table_ref[j, :, 0:width] for j in range(5))
    a, b, c = scaled_rows(up, dn, dc, an)
    for j, z in enumerate((a, b, c, sr)):
        nat_ref[j * steps : (j + 1) * steps, :] = z
    nat_ref[4 * steps : 4 * steps + ROWS, :] = an[steps - ROWS : steps, :]
    for t in range(tiles):
        price = sp_ref[start // LANES + t : start // LANES + t + 1, :]
        if t == 0:
            price = jnp.where(lane < steps, 0.0, price)
        if t == tiles - 1:
            price = jnp.where(lane >= LANES - steps, 0.0, price)
        nat_ref[4 * steps + ROWS : 4 * steps + 2 * ROWS, cols(t)] = jnp.broadcast_to(price, (ROWS, LANES))
    nat_ref[4 * steps + 2 * ROWS :, :] = jnp.zeros((LANES - 4 * steps - 2 * ROWS, width), jnp.float32)
    spread(lambda t: nat_ref[:, cols(t)], coef_ref)

    side = lax.broadcasted_iota(jnp.int32, (steps, LANES), 1)

    def joined(j):
        beyond = halo_ref[n + j * steps : n + (j + 1) * steps, :] if last else table_ref[j, :, width:seen]
        return jnp.where(side < HALF, beyond, table_ref[j, :, width - LANES : width])

    strip_an = joined(4)
    a, b, c = scaled_rows(joined(0), joined(1), joined(2), strip_an)
    if last:
        far = far_ref[0] == 1
        a = jnp.where((side == LANES - 1) & far, 0.0, a)
        c = jnp.where((side == 0) & far, 0.0, c)
    for j, z in enumerate((a, b, c, joined(3))):
        strip_ref[j * steps : (j + 1) * steps, :] = z
    strip_ref[4 * steps : 4 * steps + ROWS, :] = strip_an[steps - ROWS : steps, :]
    beyond = halo_ref[n + 5 * steps : n + 5 * steps + 1, :] if last else sp_ref[stop // LANES : stop // LANES + 1, :]
    price = jnp.where(lane < HALF, beyond, sp_ref[stop // LANES - 1 : stop // LANES, :])
    strip_ref[4 * steps + ROWS : 4 * steps + 2 * ROWS, :] = jnp.where(
        (lane < steps) | (lane >= LANES - steps), price, 0.0
    )

    def wide(ref, r, at):
        return jnp.maximum(jnp.broadcast_to(ref[r : r + 1, at], (ROWS, LANES)), -2 * OFF)

    def load(s, q, k):
        return x_ref[rows(q), cols(k)] if s == 0 else buf_ref[(s - 1) % 2, rows(q), cols(k)]

    def put_rim(s, q, first, final):
        rim_ref[s % 2, 0, rows(q), :] = pltpu.roll(first, LANES - 1, 1)
        rim_ref[s % 2, 1, rows(q), :] = pltpu.roll(final, 1, 1)

    def put_strip(s, q, e):
        e_ref[s % 2, 0, rows(q), :] = e
        e_ref[s % 2, 1, rows(q), :] = pltpu.roll(e, LANES - 1, 1)
        e_ref[s % 2, 2, rows(q), :] = pltpu.roll(e, 1, 1)

    @pl.loop(0, n // block)
    def _(i):
        all_rows = pl.ds(pl.multiple_of(i * block, block), block)
        base = [pl.ds(pl.multiple_of(i * block + ROWS * q, ROWS), ROWS) for q in range(groups)]
        pltpu.make_async_copy(
            v_ref.at[all_rows, from_start], own_ref.at[all_rows, :], own_sems.at[i]
        ).wait()
        if not last:
            pltpu.make_async_copy(
                own_ref.at[all_rows, pl.ds(0, LANES)], pack_ref.at[all_rows, :], pack_sems.at[6 + i]
            ).start()
        spread(lambda t: own_ref[all_rows, cols(t)], x_ref)
        for q in range(groups):
            put_rim(1, q, load(0, q, 0), load(0, q, tiles - 1))
            beyond = halo_ref[base[q], :] if last else own_ref[base[q], width:seen]
            put_strip(1, q, jnp.where(lane < HALF, beyond, own_ref[base[q], width - LANES : width]))
        acc = [None] * groups
        for s in range(steps):
            done = s == steps - 1
            for q0 in range(0, groups, TOGETHER):
                qs = range(q0, q0 + TOGETHER)
                terms = {q: on_terms(sgn_ref[base[q], :], key_ref[base[q], :], mask_ref[base[q], :], s) for q in qs}
                a, b, c, p = (wide(strip_ref, j * steps + s, slice(None)) for j in range(4))
                for q in qs:
                    alpha, beta = terms[q]
                    z = (s + 1) % 2
                    e = a * e_ref[z, 1, rows(q), :] + b * e_ref[z, 0, rows(q), :] + c * e_ref[z, 2, rows(q), :]
                    e = jnp.maximum(e, alpha * p - beta)
                    if done:
                        e = e * strip_ref[4 * steps + ROWS - 1 : 4 * steps + ROWS, :]
                        e_ref[s % 2, 0, rows(q), :] = e
                        acc[q] = e * strip_ref[4 * steps + ROWS : 4 * steps + 2 * ROWS, :]
                    else:
                        put_strip(s, q, e)
                below = {q: rim_ref[(s + 1) % 2, 1, rows(q), :] for q in qs}
                here = {q: load(s, q, 0) for q in qs}
                first = {}
                for k in range(tiles):
                    a, b, c, p = (wide(coef_ref, j * steps + s, cols(k)) for j in range(4))
                    if done:
                        fin = wide(coef_ref, 4 * steps + ROWS - 1, cols(k))
                        price = wide(coef_ref, 4 * steps + ROWS, cols(k))
                    for q in qs:
                        above = load(s, q, k + 1) if k + 1 < tiles else rim_ref[(s + 1) % 2, 0, rows(q), :]
                        alpha, beta = terms[q]
                        new = jnp.maximum(a * above + b * here[q] + c * below[q], alpha * p - beta)
                        below[q], here[q] = here[q], above
                        if done:
                            new = new * fin
                            x_ref[rows(q), cols(k)] = new
                            acc[q] = acc[q] + new * price
                        else:
                            buf_ref[s % 2, rows(q), cols(k)] = new
                            if k == 0:
                                first[q] = new
                            if k == tiles - 1:
                                put_rim(s, q, first[q], new)

        total = total_ref[...] if last else None
        for q in range(groups):
            if last:
                both = acc[q] + before_ref[base[q], :]
                price_ref[base[q], :] = both + pltpu.roll(both, HALF, 1)
                total = total + both
            else:
                price_ref[base[q], :] = acc[q]
        if last:
            total_ref[...] = total
        pltpu.make_async_copy(price_ref.at[all_rows, :], price_hbm.at[all_rows, :], price_sems.at[i]).start()
        for k in range(tiles):
            node_ref[pl.ds(k, LANES, stride=tiles), :] = jnp.transpose(x_ref[:, cols(k)])
        rim = lax.broadcasted_iota(jnp.int32, (block, LANES), 1)
        strip = e_ref[(steps - 1) % 2, 0]
        for t in range(tiles):
            z = jnp.transpose(node_ref[cols(t), :])
            if t == 0:
                z = jnp.where(rim < steps, strip, z)
            if t == tiles - 1:
                z = jnp.where(rim >= LANES - steps, strip, z)
            stage_ref[all_rows, cols(t)] = z
            here = pl.ds(t * LANES, LANES)
            pltpu.make_async_copy(stage_ref.at[all_rows, here], out_ref.at[all_rows, here], out_sems.at[i, t]).start()

    if last:
        total_copy = pltpu.make_async_copy(total_ref, sum_hbm, last_sems.at[1])
        total_copy.start()
    for i in range(n // block):
        at = pl.ds(i * block, block)
        pltpu.make_async_copy(price_ref.at[at, :], price_hbm.at[at, :], price_sems.at[i]).wait()
        for t in range(tiles):
            tile = pl.ds(t * LANES, LANES)
            pltpu.make_async_copy(stage_ref.at[at, tile], out_ref.at[at, tile], out_sems.at[i, t]).wait()
        if not last:
            pltpu.make_async_copy(
                own_ref.at[at, pl.ds(0, LANES)], pack_ref.at[at, :], pack_sems.at[6 + i]
            ).wait()
    for copy in pack_copies:
        copy.wait()
    if last:
        total_copy.wait()


def tail_kernel(sum_ref, *refs):
    *moved, price_ref, old_ref, out_ref, tail_ref, sem = refs
    del old_ref
    total = sum_ref[...]
    for ref in moved:
        total = total + ref[...]
    total = total + pltpu.roll(total, HALF, 1)
    lane = lax.broadcasted_iota(jnp.int32, (ROWS, LANES), 1)
    for q in range(tail_ref.shape[0] // ROWS):
        rows = slice(q * ROWS, (q + 1) * ROWS)
        tail_ref[rows, :] = jnp.where(lane < HALF, price_ref[rows, :], total)
    copy = pltpu.make_async_copy(tail_ref, out_ref.at[:, pl.ds(out_ref.shape[1] - LANES, LANES)], sem)
    copy.start()
    copy.wait()


def first_half_kernel(sources, total_width, a_ref, out_ref, sems):
    width = a_ref.shape[2]
    copies = [
        pltpu.make_async_copy(
            a_ref.at[j, :, pl.ds(LANES, width - LANES)],
            out_ref.at[:, pl.ds(j * total_width + LANES, width - LANES)],
            sems.at[j],
        )
        for j in range(sources)
    ]
    for copy in copies:
        copy.start()
    for copy in copies:
        copy.wait()


def second_half_kernel(
    sources, total_width, steps, share, a_ref, b_ref, old_ref, out_ref, price_ref, total_ref, head_ref, body_ref, sems
):
    del old_ref
    width = total_width - a_ref.shape[2]
    lane = lax.broadcasted_iota(jnp.int32, (ROWS, LANES), 1)
    copies = []
    for j in range(sources):
        left = (j + sources - 1) % sources
        at = slice(j * width, j * width + LANES)
        head_ref[:, j * LANES : (j + 1) * LANES] = jnp.where(
            lane < steps, b_ref[left, :, 0:LANES], a_ref[j, :, 0:LANES]
        )
        body_ref[:, at] = jnp.where(lane < steps, a_ref[j, :, 0:LANES], b_ref[j, :, 0:LANES])
        body_ref[:, j * width + LANES : (j + 1) * width] = b_ref[j, :, LANES:width]
        copies.append(
            pltpu.make_async_copy(
                head_ref.at[:, pl.ds(j * LANES, LANES)],
                out_ref.at[:, pl.ds(j * total_width, LANES)],
                sems.at[0, j],
            )
        )
        copies.append(
            pltpu.make_async_copy(
                body_ref.at[:, pl.ds(j * width, width)],
                out_ref.at[:, pl.ds((j + 1) * total_width - width, width)],
                sems.at[1, j],
            )
        )
        copies[-2].start()
        copies[-1].start()
    both = b_ref[0, :, width:]
    for j in range(1, sources):
        both = both + b_ref[j, :, width:]
    total_ref[0] = jnp.sum(jnp.where(lane >= HALF, both, 0.0)) / share
    mine = jnp.where(lane < HALF, both, 0.0)
    for r in range(ROWS):
        price_ref[r] = jnp.sum(mine[r : r + 1, :])
    for copy in copies:
        copy.wait()


def vmem(*shape):
    return pltpu.VMEM(shape, jnp.float32)


HERE = pl.BlockSpec(memory_space=pltpu.VMEM)
SCALARS = pl.BlockSpec(memory_space=pltpu.SMEM)
FAR = pl.BlockSpec(memory_space=pltpu.HBM)


def here(x):
    return pltpu.with_memory_space_constraint(x, pltpu.VMEM)


def roll_chunk(start, width, far, arrays, extra):
    n, total_width = arrays[0].shape
    steps = arrays[1].shape[0]
    last = start + width == total_width
    out_width = width + LANES if last else width
    seen = width if last else width + LANES
    f32 = jnp.float32
    return pl.pallas_call(
        functools.partial(roll_kernel, start, last),
        in_specs=[SCALARS] + [FAR] * len(arrays) + [HERE, FAR] * last,
        out_specs=[FAR, FAR, FAR],
        out_shape=[
            jax.ShapeDtypeStruct((n, out_width), f32),
            jax.ShapeDtypeStruct((n, LANES), f32),
            jax.ShapeDtypeStruct((ROWS if last else n + 5 * steps + ROWS, LANES), f32),
        ],
        scratch_shapes=[
            vmem(LANES, width),
            vmem(LANES, width),
            vmem(LANES, LANES),
            vmem(LANES, width),
            vmem(width, LANES),
            vmem(2, LANES, width),
            vmem(2, 2, LANES, LANES),
            vmem(2, 3, LANES, LANES),
            vmem(n, LANES),
            vmem(n, LANES),
            pltpu.VMEM((n, LANES), jnp.int32),
            vmem(n, seen),
            vmem(5, steps, seen),
            vmem(n, width),
            pltpu.SemaphoreType.DMA((5,)),
            pltpu.SemaphoreType.DMA((n // LANES,)),
            pltpu.SemaphoreType.DMA((n // LANES, width // LANES)),
        ]
        + [pltpu.VMEM(z.shape, z.dtype) for z in arrays[6:]]
        + [pltpu.SemaphoreType.DMA((5,)), vmem(n, LANES), pltpu.SemaphoreType.DMA((n // LANES,))]
        + ([vmem(n, LANES), vmem(ROWS, LANES), pltpu.SemaphoreType.DMA((2,))] if last else [pltpu.SemaphoreType.DMA((6 + n // LANES,))]),
        cost_estimate=pl.CostEstimate(
            flops=12 * n * width * steps, bytes_accessed=3 * 4 * n * width, transcendentals=0
        ),
        name="roll_last" if last else "roll_first",
    )(far, *arrays, *extra)


def local(values_in, prob_up, prob_down, discount, swap_rate, annuity, state_price, exercise_step, strike_bucket, notional_sign, strike_table):
    n, total_width = values_in.shape
    steps = prob_up.shape[0]
    node_count = lax.axis_size(NODE)
    trade_count = lax.axis_size("trade")
    rows = n // node_count
    first_width = FIRST_TILES * LANES
    second_width = total_width - first_width
    f32 = jnp.float32
    table = (prob_up, prob_down, discount, swap_rate, annuity)
    price_rows = state_price.reshape(-1, LANES)
    trades = (exercise_step.T, strike_bucket.reshape(-1, LANES), notional_sign.reshape(-1, LANES), strike_table.reshape(1, -1))

    far = (lax.axis_index(NODE) == node_count - 1).astype(jnp.int32).reshape(1)

    arrays = (values_in,) + table + (price_rows,) + trades
    first, first_sums, packed = roll_chunk(0, first_width, jnp.zeros((1,), jnp.int32), arrays, ())
    halo = lax.ppermute(packed, NODE, [((i + 1) % node_count, i) for i in range(node_count)])
    first_moved = lax.all_to_all(first.reshape(node_count, rows, first_width), NODE, 0, 0, tiled=True)
    second, part, sums = roll_chunk(first_width, second_width, far, arrays, (here(halo), first_sums))
    moved_sums = [
        lax.ppermute(sums, "trade", [(i, (i + k) % trade_count) for i in range(trade_count)])
        for k in range(1, trade_count)
    ]
    second = pl.pallas_call(
        tail_kernel,
        in_specs=[HERE] * (trade_count + 1) + [FAR],
        out_specs=FAR,
        out_shape=jax.ShapeDtypeStruct(second.shape, f32),
        scratch_shapes=[vmem(n, LANES), pltpu.SemaphoreType.DMA(())],
        input_output_aliases={trade_count + 1: 0},
        name="tail",
    )(sums, *(here(z) for z in moved_sums), part, second)
    second_moved = lax.all_to_all(
        second.reshape(node_count, rows, second_width + LANES), NODE, 0, 0, tiled=True
    )

    out_shape = jax.ShapeDtypeStruct((rows, node_count * total_width), f32)
    half = pl.pallas_call(
        functools.partial(first_half_kernel, node_count, total_width),
        in_specs=[HERE],
        out_specs=FAR,
        out_shape=out_shape,
        scratch_shapes=[pltpu.SemaphoreType.DMA((node_count,))],
        cost_estimate=pl.CostEstimate(flops=4 * n * total_width, bytes_accessed=8 * n * first_width, transcendentals=0),
        name="first_half",
    )(here(first_moved))
    values, prices, portfolio = pl.pallas_call(
        functools.partial(second_half_kernel, node_count, total_width, steps, float(n)),
        in_specs=[HERE, HERE, FAR],
        out_specs=[FAR, SCALARS, SCALARS],
        out_shape=[out_shape, jax.ShapeDtypeStruct((rows,), f32), jax.ShapeDtypeStruct((1,), f32)],
        scratch_shapes=[
            vmem(rows, node_count * LANES),
            vmem(rows, node_count * second_width),
            pltpu.SemaphoreType.DMA((2, node_count)),
        ],
        input_output_aliases={2: 0},
        name="second_half",
    )(here(first_moved), here(second_moved), half)
    return values, prices, portfolio.reshape(())


def solution(mesh):
    split = Mesh(mesh.devices.reshape(mesh.shape["trade"], 4, 4, 2), TRADE_NODE)
    in_specs = (
        P("trade", NODE),
        P(None, NODE),
        P(None, NODE),
        P(None, NODE),
        P(None, NODE),
        P(None, NODE),
        P(NODE),
        P("trade", None),
        P("trade"),
        P("trade"),
        P(),
    )
    out_specs = (P(TRADE_NODE, None), P(TRADE_NODE), P())

    return jax.shard_map(local, mesh=split, in_specs=in_specs, out_specs=out_specs, check_vma=False)
```
